128 devices in a mesh: gx: 16 (over x_hi, z, core), gy: 8 (over x_lo, y).
Axes of the slice: x: 4 (x_hi: 2, x_lo: 2; x = x_hi * 2 + x_lo), y: 4, z: 4, core: 2. Of those that a mesh axis runs over, the one named last changes fastest.
Arguments:
- theta: float32 [32, 2048, 2048], P('gx', 'gy'), may hold values from 0.9 to 1.4
- pressure: float32 [32, 2048, 2048], P('gx', 'gy'), may hold values from 0.1 to 1
- vertical_wind: float32 [32, 2048, 2048], P('gx', 'gy'), may hold values from -6 to 6
- terrain: float32 [2048, 2048], P('gx', 'gy'), may hold values from 0 to 0.5
- column_mass: float32 [2048, 2048], P('gx', 'gy'), may hold values from 0.5 to 1
- land_mask: int32 [2048, 2048], P('gx', 'gy'), may hold values 0 or 1
- pbl_top: int32 [2048, 2048], P('gx', 'gy'), may hold values from 2 to 27
Outputs:
- updated_wind: float32 [32, 2048, 2048], P(None, 'gx', 'gy')
- geopotential: float32 [32, 2048, 2048], P(None, 'gx', 'gy')
The draws below stay inside these ranges and needn't reach their ends.
All inputs are finite; a program needn't handle non-finite values. No bound on the sum of `land_mask` on one device may be relied on, other than what follows from the above.
Results may differ from the reference program's by a relative error of at most 0.00002.
Values sent between devices are 32-bit elements; how exact they have to be, the bound alone decides.
A program may use at most 128 MiB of HBM per device.

```python
import math
import jax
import jax.numpy as jnp
from jax import lax

NZ = 32
NX = 2048
NY = 2048


def place_ends(values, stream_key, least, largest):
    shape = values.shape
    place = [jax.random.randint(jax.random.fold_in(stream_key, axis), (), 0, shape[axis]) for axis in range(len(shape))]
    values = values.at[tuple(place)].set(least)
    longest = shape.index(max(shape))
    place[longest] = (place[longest] + 1) % shape[longest]
    return values.at[tuple(place)].set(largest)


def block_levels(stream_key, extent, split, least, high):
    factor_of = 1.0
    for position, shards_of in split:
        steps = jax.random.uniform(jax.random.fold_in(jax.random.fold_in(stream_key, 6), position), (shards_of,), jnp.float32, least / len(split), high / len(split))
        factor_of = factor_of * jnp.repeat(jnp.exp(steps), extent[position] // shards_of).reshape((-1,) + (1,) * (len(extent) - 1 - position))
    return factor_of


def centred(rng, dims, spread, most, pieces=(), dtype=jnp.bfloat16):
    drawn = spread * jax.random.normal(rng, dims, jnp.float32)
    if pieces:
        drawn = drawn * block_levels(rng, dims, pieces, -0.22, 0.18)
    return jnp.clip(drawn, -most, most).astype(dtype)


def setup_inputs(seed: int = 0) -> dict:
    splits = jax.random.split(jax.random.key(seed), 8)
    theta = jnp.clip(0.9 + 0.5 * jax.random.uniform(splits[0], (NZ, NX, NY), jnp.float32) ** block_levels(splits[0], (NZ, NX, NY), ((0, 16), (1, 8)), -0.2, 0.2), 0.9, 1.4)
    pressure = jnp.clip(jnp.exp(math.log(1.0) - 2.3025851 * jax.random.uniform(splits[1], (NZ, NX, NY), jnp.float32) ** block_levels(splits[1], (NZ, NX, NY), ((0, 16), (1, 8)), -0.2, 0.2)), 0.1, 1.0)
    vertical_wind = centred(splits[2], (NZ, NX, NY), 1.0, 6.0, ((0, 16), (1, 8)), jnp.float32)
    terrain = jnp.clip(0.5 * jax.random.uniform(splits[3], (NX, NY), jnp.float32) ** block_levels(splits[3], (NX, NY), ((0, 16), (1, 8)), -0.2, 0.2), 0.0, 0.5)
    column_mass = jnp.clip(0.5 + 0.5 * jax.random.uniform(splits[4], (NX, NY), jnp.float32) ** block_levels(splits[4], (NX, NY), ((0, 16), (1, 8)), -0.2, 0.2), 0.5, 1.0)
    land_mask = place_ends((jax.random.randint(splits[5], (NX, NY), 0, 2) < 1).astype(jnp.int32), jax.random.fold_in(splits[5], 1), 0, 1)
    pbl_top = place_ends(jax.random.randint(splits[6], (NX, NY), 2, NZ - 4), jax.random.fold_in(splits[6], 1), 2, (NZ - 4) - 1).astype(jnp.int32)
    return dict(theta=theta, pressure=pressure, vertical_wind=vertical_wind, terrain=terrain, column_mass=column_mass, land_mask=land_mask, pbl_top=pbl_top)


gamma_ratio = 1.4
smooth_rate = 0.2
lift_rate = 0.3
couple_rate = 0.5
land_boost = 0.5


def states(theta, pressure):
    alpha = theta * jnp.exp(-jnp.log(pressure) / gamma_ratio)
    sound_sq = gamma_ratio * pressure * alpha
    return alpha, sound_sq


def heights(terrain, column_mass, rising):
    return terrain[None] + column_mass[None] * rising / rising.shape[0]


def laplacian(padded):
    middle = padded[..., 1:-1, 1:-1]
    return padded[..., 2:, 1:-1] + padded[..., :-2, 1:-1] + padded[..., 1:-1, 2:] + padded[..., 1:-1, :-2] - 4.0 * middle


def column_solve(forcing, sound_sq, land_mask, pbl_top):
    levels = lax.broadcasted_iota(jnp.int32, forcing.shape, 0)
    inside = (land_mask[None] > 0) & (levels < pbl_top[None])
    damping = jnp.where(inside, 1.0 + land_boost, 1.0).astype(jnp.float32)
    couple = couple_rate * 0.5 * (sound_sq[:-1] + sound_sq[1:])
    zero_level = jnp.zeros_like(forcing[:1])
    below = jnp.concatenate([zero_level, couple], 0)
    above = jnp.concatenate([couple, zero_level], 0)
    centre = damping + below + above
    count = forcing.shape[0]
    ratios = []
    values = []
    ratio = above[0] / centre[0]
    value = forcing[0] / centre[0]
    ratios.append(ratio)
    values.append(value)
    for level in range(1, count):
        denom = centre[level] - below[level] * ratio
        value = (forcing[level] + below[level] * value) / denom
        ratio = above[level] / denom
        ratios.append(ratio)
        values.append(value)
    result = [None] * count
    current = values[count - 1]
    result[count - 1] = current
    for level in range(count - 2, -1, -1):
        current = values[level] + ratios[level] * current
        result[level] = current
    return jnp.stack(result, 0)


def reference(theta, pressure, vertical_wind, terrain, column_mass, land_mask, pbl_top):
    alpha, sound_sq = states(theta, pressure)
    rising = jnp.cumsum(alpha, axis=0)
    geopotential = heights(terrain, column_mass, rising)
    edges = ((0, 0), (1, 1), (1, 1))
    wind_pad = jnp.pad(vertical_wind, edges)
    geo_pad = jnp.pad(geopotential, edges)
    forcing = vertical_wind + smooth_rate * laplacian(wind_pad) + lift_rate * laplacian(geo_pad)
    updated_wind = column_solve(forcing, sound_sq, land_mask, pbl_top)
    return updated_wind, geopotential
```

```python
import functools
import jax
import jax.numpy as jnp
from jax import lax
from jax.experimental import pallas as pl
from jax.experimental.pallas import tpu as pltpu
from jax.sharding import PartitionSpec as P

gamma_ratio = 1.4
smooth_rate = 0.2
lift_rate = 0.3
couple_rate = 0.5
land_boost = 0.5


def extended(x, sides, width):
    edges = {}
    for axis, dim in sides:
        count, length = (lax.axis_size(axis), x.shape[dim])
        up = [(i, (i + 1) % count) for i in range(count - 1)]
        last = lax.slice_in_dim(x, length - width, length, axis=dim)
        initial = lax.slice_in_dim(x, 0, width, axis=dim)
        edges[dim] = (
            lax.ppermute(last, axis, up),
            lax.ppermute(initial, axis, [(b, a) for a, b in up]),
        )
    done = []
    for _, dim in sides:
        low, high = edges[dim]
        around = [(width, width) if d in done else (0, 0) for d in range(x.ndim)]
        x = jnp.concatenate([jnp.pad(low, around), x, jnp.pad(high, around)], axis=dim)
        done.append(dim)
    return x


def extended_2(x, sides, width):
    for axis, dim in sides:
        count, length = (lax.axis_size(axis), x.shape[dim])
        up = [(i, (i + 1) % count) for i in range(count - 1)]
        down = [(j, i) for i, j in up]
        last = lax.slice_in_dim(x, length - width, length, axis=dim)
        initial = lax.slice_in_dim(x, 0, width, axis=dim)
        before = lax.ppermute(last, axis, up)
        after = lax.ppermute(initial, axis, down)
        x = jnp.concatenate([before, x, after], axis=dim)
    return x


def states(theta, pressure):
    alpha = theta * jnp.exp(-jnp.log(pressure) / gamma_ratio)
    sound_sq = gamma_ratio * pressure * alpha
    return (alpha, sound_sq)


def heights(terrain, column_mass, rising):
    return terrain[None] + column_mass[None] * rising / rising.shape[0]


def laplacian(padded):
    middle = padded[..., 1:-1, 1:-1]
    return (
        padded[..., 2:, 1:-1]
        + padded[..., :-2, 1:-1]
        + padded[..., 1:-1, 2:]
        + padded[..., 1:-1, :-2]
        - 4.0 * middle
    )


def column_solve(forcing, sound_sq, land_mask, pbl_top):
    levels = lax.broadcasted_iota(jnp.int32, forcing.shape, 0)
    inside = (land_mask[None] > 0) & (levels < pbl_top[None])
    damping = jnp.where(inside, 1.0 + land_boost, 1.0).astype(jnp.float32)
    couple = couple_rate * 0.5 * (sound_sq[:-1] + sound_sq[1:])
    zero_level = jnp.zeros_like(forcing[:1])
    below = jnp.concatenate([zero_level, couple], 0)
    above = jnp.concatenate([couple, zero_level], 0)
    centre = damping + below + above
    count = forcing.shape[0]
    ratios = []
    values = []
    ratio = above[0] / centre[0]
    value = forcing[0] / centre[0]
    ratios.append(ratio)
    values.append(value)
    for level in range(1, count):
        denom = centre[level] - below[level] * ratio
        value = (forcing[level] + below[level] * value) / denom
        ratio = above[level] / denom
        ratios.append(ratio)
        values.append(value)
    result = [None] * count
    current = values[count - 1]
    result[count - 1] = current
    for level in range(count - 2, -1, -1):
        current = values[level] + ratios[level] * current
        result[level] = current
    return jnp.stack(result, 0)


PIECE = 32


def send_order(steps):
    return [
        (a, r, shift, half, core)
        for pair in range(2)
        for a in range(3)
        for r in range(steps)
        for core in range(2)
        for shift in (pair, pair + 2)
        for half in range(2)
    ]


def relay(t_in, p_in, w_in, t_out, p_out, w_out, own, send, recv, local):
    gx, gy = lax.axis_index("gx"), lax.axis_index("gy")
    ins, outs = (t_in, p_in, w_in), (t_out, p_out, w_out)
    z, c, y = (gx // 2) % 4, gx % 2, gy % 4
    stays = (gx // 2) == gy

    @pl.when(stays)
    def _():
        for a in range(3):
            rows = pl.ds(pl.multiple_of(c * 128, 128), 128)
            cols = pl.ds(pl.multiple_of(gy * 256, 256), 256)
            pltpu.make_async_copy(ins[a].at[:, rows, cols], own.at[a], local.at[a]).start()

    for a, r, shift, half, core in send_order(128 // PIECE):
        c_to = (c + core) % 2
        gy_to = half * 4 + (y + shift - z + 4) % 4
        gx_to = gy * 2 + c_to
        rows = pl.ds(pl.multiple_of(c_to * 128 + r * PIECE, PIECE), PIECE)
        cols = pl.ds(pl.multiple_of(gy_to * 256, 256), 256)

        @pl.when(jnp.logical_not((gx_to == gx) & (gy_to == gy)))
        def _():
            pltpu.make_async_remote_copy(
                ins[a].at[:, rows, cols],
                outs[a].at[pl.ds(gx * 2, 2), pl.ds(r * PIECE, PIECE)],
                send.at[a],
                recv.at[a],
                device_id={"gx": gx_to, "gy": gy_to},
                device_id_type=pl.DeviceIdType.MESH,
            ).start()

    @pl.when(stays)
    def _():
        for a in range(3):
            pltpu.make_async_copy(own.at[a], own.at[a], local.at[a]).wait()
            pltpu.make_async_copy(own.at[a], outs[a].at[pl.ds(gx * 2, 2)], local.at[a]).start()
        for a in range(3):
            pltpu.make_async_copy(own.at[a], own.at[a], local.at[a]).wait()

    for a in range(3):
        for count, cond in ((30, stays), (32, jnp.logical_not(stays))):

            @pl.when(cond)
            def _():
                whole = outs[a].at[pl.ds(0, count)]
                pltpu.make_async_copy(whole, whole, recv.at[a]).wait()
                pltpu.make_async_copy(whole, whole, send.at[a]).wait()


def to_tiles(theta, pressure, vertical_wind):
    tile = jax.ShapeDtypeStruct((32, 128, 256), jnp.float32)
    anywhere = pl.BlockSpec(memory_space=pl.ANY)
    return pl.pallas_call(
        relay,
        name="relay",
        out_shape=(tile,) * 3,
        in_specs=[anywhere] * 3,
        out_specs=(anywhere,) * 3,
        scratch_shapes=[
            pltpu.VMEM((3, 2, 128, 256), jnp.float32),
            pltpu.SemaphoreType.DMA((3,)),
            pltpu.SemaphoreType.DMA((3,)),
            pltpu.SemaphoreType.DMA((3,)),
        ],
        compiler_params=pltpu.CompilerParams(has_side_effects=True),
    )(theta, pressure, vertical_wind)


def on_device(theta, pressure, vertical_wind, terrain, column_mass, land_mask, pbl_top):
    theta_col, press_col, wind_col = to_tiles(theta, pressure, vertical_wind)
    alpha, sound_sq = states(theta_col, press_col)
    rising = jnp.cumsum(alpha, axis=0)
    wind_pad = extended(wind_col, (("gx", 1), ("gy", 2)), 1)
    geopotential = heights(terrain, column_mass, rising)
    geo_pad = extended_2(geopotential, (("gx", 1), ("gy", 2)), 1)
    forcing = wind_col + smooth_rate * laplacian(wind_pad) + lift_rate * laplacian(geo_pad)
    updated_wind = column_solve(forcing, sound_sq, land_mask, pbl_top)
    return (updated_wind, geopotential)


def solution(mesh):
    placed = (
        P("gx", "gy", None),
        P("gx", "gy", None),
        P("gx", "gy", None),
        P("gx", "gy"),
        P("gx", "gy"),
        P("gx", "gy"),
        P("gx", "gy"),
    )
    return jax.shard_map(
        on_device,
        mesh=mesh,
        in_specs=placed,
        out_specs=(P(None, "gx", "gy"), P(None, "gx", "gy")),
        check_vma=False,
    )
```

```python
import jax
import jax.numpy as jnp
from jax import lax
from jax.experimental import pallas as pl
from jax.experimental.pallas import tpu as pltpu
from jax.sharding import PartitionSpec as P

gamma_ratio = 1.4
smooth_rate = 0.2
lift_rate = 0.3
couple_rate = 0.5
land_boost = 0.5

LEVELS, ROWS, COLS = 32, 128, 256
SLAB_ROWS, SLAB_COLS = 256, 2048
PIECE = 32
BAND = 16
MIB = 1024 * 1024


def remote(src, dst, send, recv, gx, gy):
    return pltpu.make_async_remote_copy(
        src, dst, send, recv, device_id={"gx": gx, "gy": gy}, device_id_type=pl.DeviceIdType.MESH
    )


def await_bytes(ref, sem):
    pltpu.make_async_copy(ref, ref, sem).wait()


def send_pieces(srcs, dsts, sends, recvs, pair):
    gx, gy = lax.axis_index("gx"), lax.axis_index("gy")
    z, c, y = (gx // 2) % 4, gx % 2, gy % 4
    starts = []
    for a in range(len(srcs)):
        for r in range(ROWS // PIECE):
            for core in range(2):
                for shift in (pair, pair + 2):
                    for half in range(2):
                        starts.append((a, r, core, shift, half))
    for a, r, core, shift, half in starts:
        c_to = (c + core) % 2
        gx_to = gy * 2 + c_to
        gy_to = half * 4 + (y + shift - z + 4) % 4
        rows = pl.ds(pl.multiple_of(c_to * ROWS + r * PIECE, PIECE), PIECE)
        cols = pl.ds(pl.multiple_of(gy_to * COLS, COLS), COLS)

        @pl.when(jnp.logical_not((gx_to == gx) & (gy_to == gy)))
        def _():
            remote(
                srcs[a].at[:, rows, cols],
                dsts[a].at[pl.ds(gx * 2, 2), pl.ds(r * PIECE, PIECE)],
                sends[a],
                recvs[a],
                gx_to,
                gy_to,
            ).start()


def smooth_wind(wind, smoothed):
    sub = lax.broadcasted_iota(jnp.int32, (8, SLAB_COLS), 0)
    lane = lax.broadcasted_iota(jnp.int32, (8, SLAB_COLS), 1)
    for level in range(2):

        def block(b, _):
            at = pl.multiple_of(b * 8, 8)
            before = wind[level, pl.ds(at, 8), :]
            here = wind[level, pl.ds(pl.multiple_of(at + 8, 8), 8), :]
            after = wind[level, pl.ds(pl.multiple_of(at + 16, 8), 8), :]
            low = jnp.where(sub == 0, pltpu.roll(before, 1, 0), pltpu.roll(here, 1, 0))
            high = jnp.where(sub == 7, pltpu.roll(after, 7, 0), pltpu.roll(here, 7, 0))
            left = jnp.where(lane == 0, 0.0, pltpu.roll(here, 1, 1))
            right = jnp.where(lane == SLAB_COLS - 1, 0.0, pltpu.roll(here, SLAB_COLS - 1, 1))
            lap = high + low + right + left - 4.0 * here
            smoothed[level, pl.ds(at, 8), :] = here + smooth_rate * lap
            return 0

        lax.fori_loop(0, SLAB_ROWS // 8, block, 0)


def columns(theta, press, terrain, mass, land, top, geo, couple, inverse):
    def band(b, _):
        rows = pl.ds(pl.multiple_of(b * BAND, BAND), BAND)
        ground, weight = terrain[rows, :], mass[rows, :]
        limit = jnp.where(land[rows, :] > 0, top[rows, :], 0)

        def state(k, rising):
            p = press[k, rows, :]
            alpha = theta[k, rows, :] * jnp.exp(-jnp.log(p) / gamma_ratio)
            rising = rising + alpha
            geo[k, rows, :] = ground + weight * rising / LEVELS
            return rising, gamma_ratio * p * alpha

        def eliminate(k, below, above, ratio):
            damping = jnp.where(k < limit, 1.0 + land_boost, 1.0)
            denom = damping + below + above - below * ratio
            inv = 1.0 / denom
            inverse[k, rows, :] = inv
            couple[k, rows, :] = above
            return above * inv

        def level(k, carry):
            rising, sound_low, below, ratio = carry
            rising, sound = state(k, rising)
            above = couple_rate * 0.5 * (sound_low + sound)
            ratio = eliminate(k - 1, below, above, ratio)
            return rising, sound, above, ratio

        zero = jnp.zeros((BAND, COLS), jnp.float32)
        rising, sound = state(0, zero)
        _, _, below, ratio = lax.fori_loop(1, LEVELS, level, (rising, sound, zero, zero))
        eliminate(LEVELS - 1, below, zero, ratio)
        return 0

    lax.fori_loop(0, ROWS // BAND, band, 0)


def pack_columns(geo, packed):
    lane = lax.broadcasted_iota(jnp.int32, (ROWS, 128), 1)
    packed[...] = jnp.zeros_like(packed)

    def level(k, _):
        last = pltpu.roll(geo[k, :, COLS - 128 :], k + 1, 1)
        first = pltpu.roll(geo[k, :, :128], k, 1)
        packed[0] = jnp.where(lane == k, last, packed[0])
        packed[1] = jnp.where(lane == k, first, packed[1])
        return 0

    lax.fori_loop(0, LEVELS, level, 0)


def lift(geo, edge_rows, edge_cols, out):
    sub = lax.broadcasted_iota(jnp.int32, (ROWS, COLS), 0)
    lane = lax.broadcasted_iota(jnp.int32, (ROWS, 128), 1)

    def level(k, _):
        here = geo[k]
        low = jnp.where(sub == 0, edge_rows[0, k], pltpu.roll(here, 1, 0))
        high = jnp.where(sub == ROWS - 1, edge_rows[1, k], pltpu.roll(here, ROWS - 1, 0))
        left = pltpu.roll(here, 1, 1)
        right = pltpu.roll(here, COLS - 1, 1)
        from_left = pltpu.roll(edge_cols[0], 128 - k, 1)
        from_right = pltpu.roll(edge_cols[1], 127 - k, 1)
        for half in range(2):
            part = slice(half * 128, half * 128 + 128)
            l, r = left[:, part], right[:, part]
            if half == 0:
                l = jnp.where(lane == 0, from_left, l)
            else:
                r = jnp.where(lane == 127, from_right, r)
            lap = high[:, part] + low[:, part] + r + l - 4.0 * here[:, part]
            out[k, :, part] = lift_rate * lap
        return 0

    lax.fori_loop(0, LEVELS, level, 0)


def gather(
    theta_in, press_in, wind_in, terrain_in, mass_in, land_in, top_in,
    forcing, lifted, couple, inverse, geo,
    theta, press, wind, smoothed, terrain, mass, land, top,
    edge_rows, edge_cols, packed, send, recv, edge_send, edge_recv, local,
):
    gx, gy = lax.axis_index("gx"), lax.axis_index("gy")
    c = gx % 2
    stays = (gx // 2) == gy
    own_rows = pl.ds(pl.multiple_of(c * ROWS, ROWS), ROWS)
    own_cols = pl.ds(pl.multiple_of(gy * COLS, COLS), COLS)
    own_levels = pl.ds(gx * 2, 2)
    inner = pl.ds(8, SLAB_ROWS)

    wind_up = remote(
        wind_in.at[:, pl.ds(SLAB_ROWS - 1, 1), :], wind.at[:, pl.ds(7, 1), :],
        edge_send.at[0], edge_recv.at[0], gx, (gy + 1) % 8,
    )
    wind_down = remote(
        wind_in.at[:, pl.ds(0, 1), :], wind.at[:, pl.ds(8 + SLAB_ROWS, 1), :],
        edge_send.at[1], edge_recv.at[1], gx, (gy + 7) % 8,
    )
    geo_up = remote(
        geo.at[:, pl.ds(ROWS - 1, 1), :], edge_rows.at[0],
        edge_send.at[2], edge_recv.at[2], (gx + 1) % 16, gy,
    )
    geo_down = remote(
        geo.at[:, pl.ds(0, 1), :], edge_rows.at[1],
        edge_send.at[3], edge_recv.at[3], (gx + 15) % 16, gy,
    )
    geo_right = remote(
        packed.at[0], edge_cols.at[0], edge_send.at[4], edge_recv.at[4], gx, (gy + 1) % 8
    )
    geo_left = remote(
        packed.at[1], edge_cols.at[1], edge_send.at[5], edge_recv.at[5], gx, (gy + 7) % 8
    )
    low_x, high_x, low_y, high_y = gx > 0, gx < 15, gy > 0, gy < 7

    pl.when(high_y)(lambda: wind_up.start())
    pl.when(low_y)(lambda: wind_down.start())
    loads = [
        pltpu.make_async_copy(wind_in, wind.at[:, inner, :], local.at[0]),
        pltpu.make_async_copy(terrain_in, terrain, local.at[1]),
        pltpu.make_async_copy(mass_in, mass, local.at[2]),
        pltpu.make_async_copy(land_in, land, local.at[3]),
        pltpu.make_async_copy(top_in, top, local.at[4]),
    ]
    own = [
        pltpu.make_async_copy(
            src.at[:, own_rows, own_cols], dst.at[own_levels], local.at[5 + a]
        )
        for a, (src, dst) in enumerate(((theta_in, theta), (press_in, press)))
    ]
    for pair in range(2):
        send_pieces(
            (theta_in, press_in), (theta, press),
            (send.at[0], send.at[1]), (recv.at[0], recv.at[1]), pair,
        )
    for load in loads:
        load.start()

    @pl.when(stays)
    def _():
        for copy in own:
            copy.start()

    blank = jnp.zeros((1, SLAB_COLS), jnp.float32)

    @pl.when(jnp.logical_not(low_y))
    def _():
        for level in range(2):
            wind[level, pl.ds(7, 1), :] = blank

    @pl.when(jnp.logical_not(high_y))
    def _():
        for level in range(2):
            wind[level, pl.ds(8 + SLAB_ROWS, 1), :] = blank

    loads[0].wait()
    pl.when(low_y)(lambda: wind_up.wait_recv())
    pl.when(high_y)(lambda: wind_down.wait_recv())
    smooth_wind(wind, smoothed)

    @pl.when(stays)
    def _():
        for level in range(2):
            forcing[gx * 2 + level] = smoothed[level, own_rows, own_cols]

    send_pieces((smoothed,), (forcing,), (send.at[2],), (recv.at[2],), 0)

    for load in loads[1:]:
        load.wait()

    @pl.when(stays)
    def _():
        for a, dst in enumerate((theta, press)):
            own[a].wait()
            await_bytes(dst.at[pl.ds(0, LEVELS - 2)], recv.at[a])

    @pl.when(jnp.logical_not(stays))
    def _():
        for a, dst in enumerate((theta, press)):
            await_bytes(dst, recv.at[a])

    columns(theta, press, terrain, mass, land, top, geo, couple, inverse)
    pack_columns(geo, packed)

    @pl.when(jnp.logical_not(low_x))
    def _():
        edge_rows[0] = jnp.zeros((LEVELS, 1, COLS), jnp.float32)

    @pl.when(jnp.logical_not(high_x))
    def _():
        edge_rows[1] = jnp.zeros((LEVELS, 1, COLS), jnp.float32)

    @pl.when(jnp.logical_not(low_y))
    def _():
        edge_cols[0] = jnp.zeros((ROWS, 128), jnp.float32)

    @pl.when(jnp.logical_not(high_y))
    def _():
        edge_cols[1] = jnp.zeros((ROWS, 128), jnp.float32)

    pl.when(high_x)(lambda: geo_up.start())
    pl.when(low_x)(lambda: geo_down.start())
    pl.when(high_y)(lambda: geo_right.start())
    pl.when(low_y)(lambda: geo_left.start())
    send_pieces((smoothed,), (forcing,), (send.at[2],), (recv.at[2],), 1)

    pl.when(low_x)(lambda: geo_up.wait_recv())
    pl.when(high_x)(lambda: geo_down.wait_recv())
    pl.when(low_y)(lambda: geo_right.wait_recv())
    pl.when(high_y)(lambda: geo_left.wait_recv())
    lift(geo, edge_rows, edge_cols, lifted)

    for cond, copies in (
        (high_x, (geo_up,)),
        (low_x, (geo_down,)),
        (high_y, (wind_up, geo_right)),
        (low_y, (wind_down, geo_left)),
    ):

        @pl.when(cond)
        def _():
            for copy in copies:
                copy.wait_send()

    for count, cond in ((LEVELS - 2, stays), (LEVELS, jnp.logical_not(stays))):

        @pl.when(cond)
        def _():
            await_bytes(forcing.at[pl.ds(0, count)], recv.at[2])
            for a, ref in enumerate((theta, press, forcing)):
                await_bytes(ref.at[pl.ds(0, count)], send.at[a])


def finish(forcing, lifted, couple, inverse, geo_in, wind, geo_out, sem):
    step, steps = pl.program_id(0), pl.num_programs(0)
    rows = pl.ds(pl.multiple_of(step * BAND, BAND), BAND)
    copy = pltpu.make_async_copy(geo_in, geo_out, sem)
    pl.when(step == 0)(lambda: copy.start())
    value = (forcing[0, rows, :] + lifted[0, rows, :]) * inverse[0, rows, :]
    wind[0] = value
    for k in range(1, LEVELS):
        below = couple[k - 1, rows, :]
        value = (forcing[k, rows, :] + lifted[k, rows, :] + below * value) * inverse[k, rows, :]
        wind[k] = value
    for k in range(LEVELS - 2, -1, -1):
        value = wind[k] + couple[k, rows, :] * inverse[k, rows, :] * value
        wind[k] = value
    pl.when(step == steps - 1)(lambda: copy.wait())


def on_device(*args):
    tile = jax.ShapeDtypeStruct((LEVELS, ROWS, COLS), jnp.float32)
    hbm = pl.BlockSpec(memory_space=pltpu.HBM)
    vmem = pl.BlockSpec(memory_space=pltpu.VMEM)
    f32, i32 = jnp.float32, jnp.int32
    parts = pl.pallas_call(
        gather,
        name="gather",
        out_shape=(tile,) * 5,
        in_specs=[hbm] * 7,
        out_specs=(vmem,) * 5,
        scratch_shapes=[
            pltpu.VMEM((LEVELS, ROWS, COLS), f32),
            pltpu.VMEM((LEVELS, ROWS, COLS), f32),
            pltpu.VMEM((2, SLAB_ROWS + 16, SLAB_COLS), f32),
            pltpu.VMEM((2, SLAB_ROWS, SLAB_COLS), f32),
            pltpu.VMEM((ROWS, COLS), f32),
            pltpu.VMEM((ROWS, COLS), f32),
            pltpu.VMEM((ROWS, COLS), i32),
            pltpu.VMEM((ROWS, COLS), i32),
            pltpu.VMEM((2, LEVELS, 1, COLS), f32),
            pltpu.VMEM((2, ROWS, 128), f32),
            pltpu.VMEM((2, ROWS, 128), f32),
            pltpu.SemaphoreType.DMA((3,)),
            pltpu.SemaphoreType.DMA((3,)),
            pltpu.SemaphoreType.DMA((6,)),
            pltpu.SemaphoreType.DMA((6,)),
            pltpu.SemaphoreType.DMA((7,)),
        ],
        compiler_params=pltpu.CompilerParams(has_side_effects=True, vmem_limit_bytes=30 * MIB),
    )(*args)
    return pl.pallas_call(
        finish,
        name="finish",
        grid=(ROWS // BAND,),
        out_shape=(tile, tile),
        in_specs=[vmem] * 5,
        out_specs=(pl.BlockSpec((LEVELS, BAND, COLS), lambda i: (0, i, 0)), hbm),
        scratch_shapes=[pltpu.SemaphoreType.DMA],
        compiler_params=pltpu.CompilerParams(vmem_limit_bytes=8 * MIB),
    )(*parts)


def solution(mesh):
    slab, tile = P("gx", "gy", None), P("gx", "gy")
    return jax.shard_map(
        on_device,
        mesh=mesh,
        in_specs=(slab,) * 3 + (tile,) * 4,
        out_specs=(P(None, "gx", "gy"),) * 2,
        check_vma=False,
    )
```

```python
import jax
import jax.numpy as jnp
from jax import lax
from jax.experimental import pallas as pl
from jax.experimental.pallas import tpu as pltpu
from jax.sharding import PartitionSpec as P

gamma_ratio = 1.4
smooth_rate = 0.2
lift_rate = 0.3
couple_rate = 0.5
land_boost = 0.5

LEVELS, ROWS, COLS = 32, 128, 256
SLAB_ROWS, SLAB_COLS = 256, 2048
PIECE = 16
BAND = 16
MIB = 1024 * 1024


def remote(src, dst, send, recv, gx, gy):
    return pltpu.make_async_remote_copy(
        src, dst, send, recv, device_id={"gx": gx, "gy": gy}, device_id_type=pl.DeviceIdType.MESH
    )


def await_bytes(ref, sem):
    pltpu.make_async_copy(ref, ref, sem).wait()


def send_pieces(srcs, dsts, sends, recvs, shifts, first, last):
    gx, gy = lax.axis_index("gx"), lax.axis_index("gy")
    z, c, y = (gx // 2) % 4, gx % 2, gy % 4

    def piece(r, _):
        for a in range(len(srcs)):
            for core in range(2):
                for shift in shifts:
                    for half in range(2):
                        c_to = (c + core) % 2
                        gx_to = gy * 2 + c_to
                        gy_to = half * 4 + (y + shift - z + 4) % 4
                        rows = pl.ds(pl.multiple_of(c_to * ROWS + r * PIECE, PIECE), PIECE)
                        cols = pl.ds(pl.multiple_of(gy_to * COLS, COLS), COLS)

                        @pl.when(jnp.logical_not((gx_to == gx) & (gy_to == gy)))
                        def _():
                            remote(
                                srcs[a].at[:, rows, cols],
                                dsts[a].at[pl.ds(gx * 2, 2), pl.ds(pl.multiple_of(r * PIECE, PIECE), PIECE)],
                                sends[a],
                                recvs[a],
                                gx_to,
                                gy_to,
                            ).start()
        return 0

    count = ROWS // PIECE
    lax.fori_loop(count * first // 4, count * last // 4, piece, 0)


def smooth_wind(wind, smoothed):
    sub = lax.broadcasted_iota(jnp.int32, (8, SLAB_COLS), 0)
    lane = lax.broadcasted_iota(jnp.int32, (8, SLAB_COLS), 1)
    for level in range(2):

        def block(b, _):
            at = pl.multiple_of(b * 8, 8)
            before = wind[level, pl.ds(at, 8), :]
            here = wind[level, pl.ds(pl.multiple_of(at + 8, 8), 8), :]
            after = wind[level, pl.ds(pl.multiple_of(at + 16, 8), 8), :]
            low = jnp.where(sub == 0, pltpu.roll(before, 1, 0), pltpu.roll(here, 1, 0))
            high = jnp.where(sub == 7, pltpu.roll(after, 7, 0), pltpu.roll(here, 7, 0))
            left = jnp.where(lane == 0, 0.0, pltpu.roll(here, 1, 1))
            right = jnp.where(lane == SLAB_COLS - 1, 0.0, pltpu.roll(here, SLAB_COLS - 1, 1))
            lap = high + low + right + left - 4.0 * here
            smoothed[level, pl.ds(at, 8), :] = here + smooth_rate * lap
            return 0

        lax.fori_loop(0, SLAB_ROWS // 8, block, 0)


def columns(theta, press, terrain, mass, land, top, geo, couple, inverse):
    def band(b, _):
        rows = pl.ds(pl.multiple_of(b * BAND, BAND), BAND)
        ground, weight = terrain[rows, :], mass[rows, :]
        limit = jnp.where(land[rows, :] > 0, top[rows, :], 0)

        def state(k, rising):
            p = press[k, rows, :]
            alpha = theta[k, rows, :] * jnp.exp(-jnp.log(p) / gamma_ratio)
            rising = rising + alpha
            geo[k, rows, :] = ground + weight * rising / LEVELS
            return rising, gamma_ratio * p * alpha

        def eliminate(k, below, above, ratio):
            damping = jnp.where(k < limit, 1.0 + land_boost, 1.0)
            denom = damping + below + above - below * ratio
            inv = 1.0 / denom
            inverse[k, rows, :] = inv
            couple[k, rows, :] = above
            return above * inv

        def level(k, carry):
            rising, sound_low, below, ratio = carry
            rising, sound = state(k, rising)
            above = couple_rate * 0.5 * (sound_low + sound)
            ratio = eliminate(k - 1, below, above, ratio)
            return rising, sound, above, ratio

        zero = jnp.zeros((BAND, COLS), jnp.float32)
        rising, sound = state(0, zero)
        _, _, below, ratio = lax.fori_loop(1, LEVELS, level, (rising, sound, zero, zero))
        eliminate(LEVELS - 1, below, zero, ratio)
        return 0

    lax.fori_loop(0, ROWS // BAND, band, 0)


def pack_columns(geo, packed):
    lane = lax.broadcasted_iota(jnp.int32, (ROWS, 128), 1)
    packed[...] = jnp.zeros_like(packed)

    def level(k, _):
        last = pltpu.roll(geo[k, :, COLS - 128 :], k + 1, 1)
        first = pltpu.roll(geo[k, :, :128], k, 1)
        packed[0] = jnp.where(lane == k, last, packed[0])
        packed[1] = jnp.where(lane == k, first, packed[1])
        return 0

    lax.fori_loop(0, LEVELS, level, 0)


def lift(geo, edge_rows, edge_cols, out):
    sub = lax.broadcasted_iota(jnp.int32, (ROWS, COLS), 0)
    lane = lax.broadcasted_iota(jnp.int32, (ROWS, 128), 1)

    def level(k, _):
        here = geo[k]
        low = jnp.where(sub == 0, edge_rows[0, k], pltpu.roll(here, 1, 0))
        high = jnp.where(sub == ROWS - 1, edge_rows[1, k], pltpu.roll(here, ROWS - 1, 0))
        left = pltpu.roll(here, 1, 1)
        right = pltpu.roll(here, COLS - 1, 1)
        from_left = pltpu.roll(edge_cols[0], 128 - k, 1)
        from_right = pltpu.roll(edge_cols[1], 127 - k, 1)
        for half in range(2):
            part = slice(half * 128, half * 128 + 128)
            l, r = left[:, part], right[:, part]
            if half == 0:
                l = jnp.where(lane == 0, from_left, l)
            else:
                r = jnp.where(lane == 127, from_right, r)
            lap = high[:, part] + low[:, part] + r + l - 4.0 * here[:, part]
            out[k, :, part] = lift_rate * lap
        return 0

    lax.fori_loop(0, LEVELS, level, 0)


def gather(
    theta_in, press_in, wind_in, terrain_in, mass_in, land_in, top_in,
    forcing, lifted, couple, inverse, geo,
    theta, press, wind, smoothed, terrain, mass, land, top,
    edge_rows, edge_cols, packed, send, recv, edge_send, edge_recv, local,
):
    gx, gy = lax.axis_index("gx"), lax.axis_index("gy")
    c = gx % 2
    stays = (gx // 2) == gy
    own_rows = pl.ds(pl.multiple_of(c * ROWS, ROWS), ROWS)
    own_cols = pl.ds(pl.multiple_of(gy * COLS, COLS), COLS)
    own_levels = pl.ds(gx * 2, 2)
    inner = pl.ds(8, SLAB_ROWS)

    wind_up = remote(
        wind_in.at[:, pl.ds(SLAB_ROWS - 1, 1), :], wind.at[:, pl.ds(7, 1), :],
        edge_send.at[0], edge_recv.at[0], gx, (gy + 1) % 8,
    )
    wind_down = remote(
        wind_in.at[:, pl.ds(0, 1), :], wind.at[:, pl.ds(8 + SLAB_ROWS, 1), :],
        edge_send.at[1], edge_recv.at[1], gx, (gy + 7) % 8,
    )
    geo_up = remote(
        geo.at[:, pl.ds(ROWS - 1, 1), :], edge_rows.at[0],
        edge_send.at[2], edge_recv.at[2], (gx + 1) % 16, gy,
    )
    geo_down = remote(
        geo.at[:, pl.ds(0, 1), :], edge_rows.at[1],
        edge_send.at[3], edge_recv.at[3], (gx + 15) % 16, gy,
    )
    geo_right = remote(
        packed.at[0], edge_cols.at[0], edge_send.at[4], edge_recv.at[4], gx, (gy + 1) % 8
    )
    geo_left = remote(
        packed.at[1], edge_cols.at[1], edge_send.at[5], edge_recv.at[5], gx, (gy + 7) % 8
    )
    low_x, high_x, low_y, high_y = gx > 0, gx < 15, gy > 0, gy < 7

    pl.when(high_y)(lambda: wind_up.start())
    pl.when(low_y)(lambda: wind_down.start())
    loads = [
        pltpu.make_async_copy(wind_in, wind.at[:, inner, :], local.at[0]),
        pltpu.make_async_copy(terrain_in, terrain, local.at[1]),
        pltpu.make_async_copy(mass_in, mass, local.at[2]),
        pltpu.make_async_copy(land_in, land, local.at[3]),
        pltpu.make_async_copy(top_in, top, local.at[4]),
    ]
    own = [
        pltpu.make_async_copy(
            src.at[:, own_rows, own_cols], dst.at[own_levels], local.at[5 + a]
        )
        for a, (src, dst) in enumerate(((theta_in, theta), (press_in, press)))
    ]
    for load in loads:
        load.start()

    @pl.when(stays)
    def _():
        for copy in own:
            copy.start()

    send_pieces((theta_in, press_in), (theta, press), (send.at[0], send.at[1]), (recv.at[0], recv.at[1]), (0, 2, 1, 3), 0, 1)
    blank = jnp.zeros((1, SLAB_COLS), jnp.float32)

    @pl.when(jnp.logical_not(low_y))
    def _():
        for level in range(2):
            wind[level, pl.ds(7, 1), :] = blank

    @pl.when(jnp.logical_not(high_y))
    def _():
        for level in range(2):
            wind[level, pl.ds(8 + SLAB_ROWS, 1), :] = blank

    loads[0].wait()
    pl.when(low_y)(lambda: wind_up.wait_recv())
    pl.when(high_y)(lambda: wind_down.wait_recv())
    smooth_wind(wind, smoothed)

    @pl.when(stays)
    def _():
        for level in range(2):
            forcing[gx * 2 + level] = smoothed[level, own_rows, own_cols]

    send_pieces((theta_in, press_in), (theta, press), (send.at[0], send.at[1]), (recv.at[0], recv.at[1]), (0, 2, 1, 3), 1, 4)
    send_pieces((smoothed,), (forcing,), (send.at[2],), (recv.at[2],), (0, 2, 1, 3), 0, 4)

    for load in loads[1:]:
        load.wait()

    @pl.when(stays)
    def _():
        for a, dst in enumerate((theta, press)):
            own[a].wait()
            await_bytes(dst.at[pl.ds(0, LEVELS - 2)], recv.at[a])

    @pl.when(jnp.logical_not(stays))
    def _():
        for a, dst in enumerate((theta, press)):
            await_bytes(dst, recv.at[a])

    columns(theta, press, terrain, mass, land, top, geo, couple, inverse)
    pack_columns(geo, packed)

    @pl.when(jnp.logical_not(low_x))
    def _():
        edge_rows[0] = jnp.zeros((LEVELS, 1, COLS), jnp.float32)

    @pl.when(jnp.logical_not(high_x))
    def _():
        edge_rows[1] = jnp.zeros((LEVELS, 1, COLS), jnp.float32)

    @pl.when(jnp.logical_not(low_y))
    def _():
        edge_cols[0] = jnp.zeros((ROWS, 128), jnp.float32)

    @pl.when(jnp.logical_not(high_y))
    def _():
        edge_cols[1] = jnp.zeros((ROWS, 128), jnp.float32)

    pl.when(high_x)(lambda: geo_up.start())
    pl.when(low_x)(lambda: geo_down.start())
    pl.when(high_y)(lambda: geo_right.start())
    pl.when(low_y)(lambda: geo_left.start())

    pl.when(low_x)(lambda: geo_up.wait_recv())
    pl.when(high_x)(lambda: geo_down.wait_recv())
    pl.when(low_y)(lambda: geo_right.wait_recv())
    pl.when(high_y)(lambda: geo_left.wait_recv())
    lift(geo, edge_rows, edge_cols, lifted)

    for cond, copies in (
        (high_x, (geo_up,)),
        (low_x, (geo_down,)),
        (high_y, (wind_up, geo_right)),
        (low_y, (wind_down, geo_left)),
    ):

        @pl.when(cond)
        def _():
            for copy in copies:
                copy.wait_send()

    for count, cond in ((LEVELS - 2, stays), (LEVELS, jnp.logical_not(stays))):

        @pl.when(cond)
        def _():
            await_bytes(forcing.at[pl.ds(0, count)], recv.at[2])
            for a, ref in enumerate((theta, press, forcing)):
                await_bytes(ref.at[pl.ds(0, count)], send.at[a])


def finish(forcing, lifted, couple, inverse, geo_in, wind, geo_out, sem):
    step, steps = pl.program_id(0), pl.num_programs(0)
    rows = pl.ds(pl.multiple_of(step * BAND, BAND), BAND)
    copy = pltpu.make_async_copy(geo_in, geo_out, sem)
    pl.when(step == 0)(lambda: copy.start())
    value = (forcing[0, rows, :] + lifted[0, rows, :]) * inverse[0, rows, :]
    wind[0] = value
    for k in range(1, LEVELS):
        below = couple[k - 1, rows, :]
        value = (forcing[k, rows, :] + lifted[k, rows, :] + below * value) * inverse[k, rows, :]
        wind[k] = value
    for k in range(LEVELS - 2, -1, -1):
        value = wind[k] + couple[k, rows, :] * inverse[k, rows, :] * value
        wind[k] = value
    pl.when(step == steps - 1)(lambda: copy.wait())


def on_device(*args):
    tile = jax.ShapeDtypeStruct((LEVELS, ROWS, COLS), jnp.float32)
    hbm = pl.BlockSpec(memory_space=pltpu.HBM)
    vmem = pl.BlockSpec(memory_space=pltpu.VMEM)
    f32, i32 = jnp.float32, jnp.int32
    parts = pl.pallas_call(
        gather,
        name="gather",
        out_shape=(tile,) * 5,
        in_specs=[hbm] * 7,
        out_specs=(vmem,) * 5,
        scratch_shapes=[
            pltpu.VMEM((LEVELS, ROWS, COLS), f32),
            pltpu.VMEM((LEVELS, ROWS, COLS), f32),
            pltpu.VMEM((2, SLAB_ROWS + 16, SLAB_COLS), f32),
            pltpu.VMEM((2, SLAB_ROWS, SLAB_COLS), f32),
            pltpu.VMEM((ROWS, COLS), f32),
            pltpu.VMEM((ROWS, COLS), f32),
            pltpu.VMEM((ROWS, COLS), i32),
            pltpu.VMEM((ROWS, COLS), i32),
            pltpu.VMEM((2, LEVELS, 1, COLS), f32),
            pltpu.VMEM((2, ROWS, 128), f32),
            pltpu.VMEM((2, ROWS, 128), f32),
            pltpu.SemaphoreType.DMA((3,)),
            pltpu.SemaphoreType.DMA((3,)),
            pltpu.SemaphoreType.DMA((6,)),
            pltpu.SemaphoreType.DMA((6,)),
            pltpu.SemaphoreType.DMA((7,)),
        ],
        compiler_params=pltpu.CompilerParams(has_side_effects=True, vmem_limit_bytes=30 * MIB),
    )(*args)
    return pl.pallas_call(
        finish,
        name="finish",
        grid=(ROWS // BAND,),
        out_shape=(tile, tile),
        in_specs=[vmem] * 5,
        out_specs=(pl.BlockSpec((LEVELS, BAND, COLS), lambda i: (0, i, 0)), hbm),
        scratch_shapes=[pltpu.SemaphoreType.DMA],
        compiler_params=pltpu.CompilerParams(vmem_limit_bytes=8 * MIB),
    )(*parts)


def solution(mesh):
    slab, tile = P("gx", "gy", None), P("gx", "gy")
    return jax.shard_map(
        on_device,
        mesh=mesh,
        in_specs=(slab,) * 3 + (tile,) * 4,
        out_specs=(P(None, "gx", "gy"),) * 2,
        check_vma=False,
    )
```

```python
import jax
import jax.numpy as jnp
from jax import lax
from jax.experimental import pallas as pl
from jax.experimental.pallas import tpu as pltpu
from jax.sharding import PartitionSpec as P

gamma_ratio = 1.4
smooth_rate = 0.2
lift_rate = 0.3
couple_rate = 0.5
land_boost = 0.5

LEVELS, ROWS, COLS = 32, 128, 256
SLAB_ROWS, SLAB_COLS = 256, 2048
PIECE = 16
BAND = 16
QUARTER = ROWS // 4
EARLY = 2
MIB = 1024 * 1024
GATHER_MIB = 44


def remote(src, dst, send, recv, gx, gy):
    return pltpu.make_async_remote_copy(
        src, dst, send, recv, device_id={"gx": gx, "gy": gy}, device_id_type=pl.DeviceIdType.MESH
    )


def await_bytes(ref, sem):
    pltpu.make_async_copy(ref, ref, sem).wait()


def send_quarter(srcs, dsts, sends, recvs, quarter):
    gx, gy = lax.axis_index("gx"), lax.axis_index("gy")
    z, c, y = (gx // 2) % 4, gx % 2, gy % 4

    def piece(r, _):
        at = pl.multiple_of(r * PIECE, PIECE)
        for a in range(len(srcs)):
            for core in range(2):
                for shift in (0, 2, 1, 3):
                    for half in range(2):
                        c_to = (c + core) % 2
                        gx_to = gy * 2 + c_to
                        gy_to = half * 4 + (y + shift - z + 4) % 4
                        rows = pl.ds(pl.multiple_of(c_to * ROWS + at, PIECE), PIECE)
                        cols = pl.ds(pl.multiple_of(gy_to * COLS, COLS), COLS)

                        @pl.when(jnp.logical_not((gx_to == gx) & (gy_to == gy)))
                        def _():
                            remote(
                                srcs[a].at[:, rows, cols],
                                dsts[a].at[pl.ds(gx * 2, 2), pl.ds(at, PIECE)],
                                sends[a],
                                recvs[a],
                                gx_to,
                                gy_to,
                            ).start()
        return 0

    count = QUARTER // PIECE
    lax.fori_loop(quarter * count, quarter * count + count, piece, 0)


def smooth_wind(wind, smoothed):
    sub = lax.broadcasted_iota(jnp.int32, (8, SLAB_COLS), 0)
    lane = lax.broadcasted_iota(jnp.int32, (8, SLAB_COLS), 1)
    for level in range(2):

        def block(b, _):
            at = pl.multiple_of(b * 8, 8)
            before = wind[level, pl.ds(at, 8), :]
            here = wind[level, pl.ds(pl.multiple_of(at + 8, 8), 8), :]
            after = wind[level, pl.ds(pl.multiple_of(at + 16, 8), 8), :]
            low = jnp.where(sub == 0, pltpu.roll(before, 1, 0), pltpu.roll(here, 1, 0))
            high = jnp.where(sub == 7, pltpu.roll(after, 7, 0), pltpu.roll(here, 7, 0))
            left = jnp.where(lane == 0, 0.0, pltpu.roll(here, 1, 1))
            right = jnp.where(lane == SLAB_COLS - 1, 0.0, pltpu.roll(here, SLAB_COLS - 1, 1))
            lap = high + low + right + left - 4.0 * here
            smoothed[level, pl.ds(at, 8), :] = here + smooth_rate * lap
            return 0

        lax.fori_loop(0, SLAB_ROWS // 8, block, 0)


def columns(theta, press, terrain, mass, land, top, geo, couple, inverse, quarter):
    def band(b, _):
        rows = pl.ds(pl.multiple_of(b * BAND, BAND), BAND)
        ground, weight = terrain[rows, :], mass[rows, :]
        limit = jnp.where(land[rows, :] > 0, top[rows, :], 0)

        def state(k, rising):
            p = press[k, rows, :]
            alpha = theta[k, rows, :] * jnp.exp(-jnp.log(p) / gamma_ratio)
            rising = rising + alpha
            geo[k, rows, :] = ground + weight * rising / LEVELS
            return rising, gamma_ratio * p * alpha

        def eliminate(k, below, above, ratio):
            damping = jnp.where(k < limit, 1.0 + land_boost, 1.0)
            denom = damping + below + above - below * ratio
            inv = 1.0 / denom
            inverse[k, rows, :] = inv
            couple[k, rows, :] = above
            return above * inv

        def level(k, carry):
            rising, sound_low, below, ratio = carry
            rising, sound = state(k, rising)
            above = couple_rate * 0.5 * (sound_low + sound)
            ratio = eliminate(k - 1, below, above, ratio)
            return rising, sound, above, ratio

        zero = jnp.zeros((BAND, COLS), jnp.float32)
        rising, sound = state(0, zero)
        _, _, below, ratio = lax.fori_loop(1, LEVELS, level, (rising, sound, zero, zero))
        eliminate(LEVELS - 1, below, zero, ratio)
        return 0

    count = QUARTER // BAND
    lax.fori_loop(quarter * count, quarter * count + count, band, 0)


def pack_columns(geo, packed, quarter):
    rows = pl.ds(quarter * QUARTER, QUARTER)
    lane = lax.broadcasted_iota(jnp.int32, (QUARTER, 128), 1)

    def level(k, carry):
        last = pltpu.roll(geo[k, rows, COLS - 128 :], k + 1, 1)
        first = pltpu.roll(geo[k, rows, :128], k, 1)
        return jnp.where(lane == k, last, carry[0]), jnp.where(lane == k, first, carry[1])

    zero = jnp.zeros((QUARTER, 128), jnp.float32)
    last, first = lax.fori_loop(0, LEVELS, level, (zero, zero))
    packed[0, rows, :] = last
    packed[1, rows, :] = first


def lift(geo, edge_rows, edge_cols, out):
    sub = lax.broadcasted_iota(jnp.int32, (ROWS, COLS), 0)
    lane = lax.broadcasted_iota(jnp.int32, (ROWS, 128), 1)

    def level(k, _):
        here = geo[k]
        low = jnp.where(sub == 0, edge_rows[0, k], pltpu.roll(here, 1, 0))
        high = jnp.where(sub == ROWS - 1, edge_rows[1, k], pltpu.roll(here, ROWS - 1, 0))
        left = pltpu.roll(here, 1, 1)
        right = pltpu.roll(here, COLS - 1, 1)
        from_left = pltpu.roll(edge_cols[0], 128 - k, 1)
        from_right = pltpu.roll(edge_cols[1], 127 - k, 1)
        for half in range(2):
            part = slice(half * 128, half * 128 + 128)
            l, r = left[:, part], right[:, part]
            if half == 0:
                l = jnp.where(lane == 0, from_left, l)
            else:
                r = jnp.where(lane == 127, from_right, r)
            lap = high[:, part] + low[:, part] + r + l - 4.0 * here[:, part]
            out[k, :, part] = lift_rate * lap
        return 0

    lax.fori_loop(0, LEVELS, level, 0)


def solve(wind, lifted, couple, inverse, quarter):
    rows = pl.ds(quarter * QUARTER, QUARTER)
    value = (wind[0, rows, :] + lifted[0, rows, :]) * inverse[0, rows, :]
    wind[0, rows, :] = value
    for k in range(1, LEVELS):
        below = couple[k - 1, rows, :]
        value = (wind[k, rows, :] + lifted[k, rows, :] + below * value) * inverse[k, rows, :]
        wind[k, rows, :] = value
    for k in range(LEVELS - 2, -1, -1):
        value = wind[k, rows, :] + couple[k, rows, :] * inverse[k, rows, :] * value
        wind[k, rows, :] = value


def gather(
    theta_in, press_in, wind_in, terrain_in, mass_in, land_in, top_in,
    forcing, geo,
    theta, press, wind, smoothed, lifted, couple, inverse, terrain, mass, land, top,
    edge_rows, edge_cols, packed, send, recv, edge_send, edge_recv, local,
):
    gx, gy = lax.axis_index("gx"), lax.axis_index("gy")
    c = gx % 2
    stays = (gx // 2) == gy
    moves = jnp.logical_not(stays)
    own_rows = pl.ds(pl.multiple_of(c * ROWS, ROWS), ROWS)
    own_cols = pl.ds(pl.multiple_of(gy * COLS, COLS), COLS)
    own_levels = pl.ds(gx * 2, 2)
    quarters = [pl.ds(q * QUARTER, QUARTER) for q in range(4)]
    low_x, high_x, low_y, high_y = gx > 0, gx < 15, gy > 0, gy < 7

    wind_up = remote(
        wind_in.at[:, pl.ds(SLAB_ROWS - 1, 1), :], wind.at[:, pl.ds(7, 1), :],
        edge_send.at[0], edge_recv.at[0], gx, (gy + 1) % 8,
    )
    wind_down = remote(
        wind_in.at[:, pl.ds(0, 1), :], wind.at[:, pl.ds(8 + SLAB_ROWS, 1), :],
        edge_send.at[1], edge_recv.at[1], gx, (gy + 7) % 8,
    )
    geo_up = remote(
        geo.at[:, pl.ds(ROWS - 1, 1), :], edge_rows.at[0],
        edge_send.at[2], edge_recv.at[2], (gx + 1) % 16, gy,
    )
    geo_down = remote(
        geo.at[:, pl.ds(0, 1), :], edge_rows.at[1],
        edge_send.at[3], edge_recv.at[3], (gx + 15) % 16, gy,
    )
    geo_right = [
        remote(
            packed.at[0, rows], edge_cols.at[0, rows],
            edge_send.at[4 + q], edge_recv.at[4 + q], gx, (gy + 1) % 8,
        )
        for q, rows in enumerate(quarters)
    ]
    geo_left = [
        remote(
            packed.at[1, rows], edge_cols.at[1, rows],
            edge_send.at[8 + q], edge_recv.at[8 + q], gx, (gy + 7) % 8,
        )
        for q, rows in enumerate(quarters)
    ]

    pl.when(high_y)(lambda: wind_up.start())
    pl.when(low_y)(lambda: wind_down.start())
    loads = [
        pltpu.make_async_copy(wind_in, wind.at[:, pl.ds(8, SLAB_ROWS), :], local.at[0]),
        pltpu.make_async_copy(terrain_in, terrain, local.at[1]),
        pltpu.make_async_copy(mass_in, mass, local.at[2]),
        pltpu.make_async_copy(land_in, land, local.at[3]),
        pltpu.make_async_copy(top_in, top, local.at[4]),
    ]
    own = [
        pltpu.make_async_copy(
            src.at[:, own_rows, own_cols], dst.at[own_levels], local.at[5 + a]
        )
        for a, (src, dst) in enumerate(((theta_in, theta), (press_in, press)))
    ]
    for load in loads:
        load.start()

    @pl.when(stays)
    def _():
        for copy in own:
            copy.start()

    def send_state(q):
        send_quarter(
            (theta_in, press_in), (theta, press),
            (send.at[0], send.at[1]), (recv.at[q], recv.at[4 + q]), q,
        )

    def send_forcing(q):
        send_quarter((smoothed,), (forcing,), (send.at[2],), (recv.at[8 + q],), q)

    def await_quarter(refs, q):
        for count, cond in ((LEVELS - 2, stays), (LEVELS, moves)):

            @pl.when(cond)
            def _():
                for a, ref in refs:
                    await_bytes(ref.at[pl.ds(0, count), quarters[q]], recv.at[4 * a + q])

    send_state(0)

    blank = jnp.zeros((1, SLAB_COLS), jnp.float32)

    @pl.when(jnp.logical_not(low_y))
    def _():
        for level in range(2):
            wind[level, pl.ds(7, 1), :] = blank
        edge_cols[0] = jnp.zeros((ROWS, 128), jnp.float32)

    @pl.when(jnp.logical_not(high_y))
    def _():
        for level in range(2):
            wind[level, pl.ds(8 + SLAB_ROWS, 1), :] = blank
        edge_cols[1] = jnp.zeros((ROWS, 128), jnp.float32)

    @pl.when(jnp.logical_not(low_x))
    def _():
        edge_rows[0] = jnp.zeros((LEVELS, 1, COLS), jnp.float32)

    @pl.when(jnp.logical_not(high_x))
    def _():
        edge_rows[1] = jnp.zeros((LEVELS, 1, COLS), jnp.float32)

    loads[0].wait()
    pl.when(low_y)(lambda: wind_up.wait_recv())
    pl.when(high_y)(lambda: wind_down.wait_recv())
    smooth_wind(wind, smoothed)

    @pl.when(stays)
    def _():
        for level in range(2):
            forcing[gx * 2 + level] = smoothed[level, own_rows, own_cols]

    for q in range(1, 4):
        send_state(q)
    for q in range(EARLY):
        send_forcing(q)

    for load in loads[1:]:
        load.wait()

    @pl.when(stays)
    def _():
        for copy in own:
            copy.wait()

    for q in range(4):
        await_quarter(((0, theta), (1, press)), q)
        columns(theta, press, terrain, mass, land, top, geo, couple, inverse, q)
        pack_columns(geo, packed, q)
        if q == 0:
            pl.when(low_x)(lambda: geo_down.start())
        if q == 3:
            pl.when(high_x)(lambda: geo_up.start())
        pl.when(high_y)(lambda: geo_right[q].start())
        pl.when(low_y)(lambda: geo_left[q].start())

    for q in range(EARLY, 4):
        send_forcing(q)

    pl.when(low_x)(lambda: geo_up.wait_recv())
    pl.when(high_x)(lambda: geo_down.wait_recv())

    @pl.when(low_y)
    def _():
        for copy in geo_right:
            copy.wait_recv()

    @pl.when(high_y)
    def _():
        for copy in geo_left:
            copy.wait_recv()

    lift(geo, edge_rows, edge_cols, lifted)
    for q in range(4):
        await_quarter(((2, forcing),), q)
        solve(forcing, lifted, couple, inverse, q)

    for cond, copies in (
        (high_x, (geo_up,)),
        (low_x, (geo_down,)),
        (high_y, (wind_up, *geo_right)),
        (low_y, (wind_down, *geo_left)),
    ):

        @pl.when(cond)
        def _():
            for copy in copies:
                copy.wait_send()

    for count, cond in ((LEVELS - 2, stays), (LEVELS, moves)):

        @pl.when(cond)
        def _():
            for a, ref in enumerate((theta, press, forcing)):
                await_bytes(ref.at[pl.ds(0, count)], send.at[a])


def store(wind, geo, wind_out, geo_out, sems):
    copies = []
    for n, (src, dst) in enumerate(((wind, wind_out), (geo, geo_out))):
        for part in range(4):
            levels = pl.ds(part * 8, 8)
            copies.append(pltpu.make_async_copy(src.at[levels], dst.at[levels], sems.at[n, part]))
    for copy in copies:
        copy.start()
    for copy in copies:
        copy.wait()


def on_device(*args):
    tile = jax.ShapeDtypeStruct((LEVELS, ROWS, COLS), jnp.float32)
    hbm = pl.BlockSpec(memory_space=pltpu.HBM)
    vmem = pl.BlockSpec(memory_space=pltpu.VMEM)
    f32, i32 = jnp.float32, jnp.int32
    parts = pl.pallas_call(
        gather,
        name="gather",
        out_shape=(tile,) * 2,
        in_specs=[hbm] * 7,
        out_specs=(vmem,) * 2,
        scratch_shapes=[
            pltpu.VMEM((LEVELS, ROWS, COLS), f32),
            pltpu.VMEM((LEVELS, ROWS, COLS), f32),
            pltpu.VMEM((2, SLAB_ROWS + 16, SLAB_COLS), f32),
            pltpu.VMEM((2, SLAB_ROWS, SLAB_COLS), f32),
            pltpu.VMEM((LEVELS, ROWS, COLS), f32),
            pltpu.VMEM((LEVELS, ROWS, COLS), f32),
            pltpu.VMEM((LEVELS, ROWS, COLS), f32),
            pltpu.VMEM((ROWS, COLS), f32),
            pltpu.VMEM((ROWS, COLS), f32),
            pltpu.VMEM((ROWS, COLS), i32),
            pltpu.VMEM((ROWS, COLS), i32),
            pltpu.VMEM((2, LEVELS, 1, COLS), f32),
            pltpu.VMEM((2, ROWS, 128), f32),
            pltpu.VMEM((2, ROWS, 128), f32),
            pltpu.SemaphoreType.DMA((3,)),
            pltpu.SemaphoreType.DMA((12,)),
            pltpu.SemaphoreType.DMA((12,)),
            pltpu.SemaphoreType.DMA((12,)),
            pltpu.SemaphoreType.DMA((7,)),
        ],
        compiler_params=pltpu.CompilerParams(
            has_side_effects=True, vmem_limit_bytes=GATHER_MIB * MIB
        ),
    )(*(pltpu.with_memory_space_constraint(x, pltpu.HBM) for x in args))
    return pl.pallas_call(
        store,
        name="store",
        out_shape=(tile, tile),
        in_specs=[vmem] * 2,
        out_specs=(hbm, hbm),
        scratch_shapes=[pltpu.SemaphoreType.DMA((2, 4))],
        compiler_params=pltpu.CompilerParams(vmem_limit_bytes=1 * MIB),
    )(*parts)


def solution(mesh):
    slab, tile = P("gx", "gy", None), P("gx", "gy")
    return jax.shard_map(
        on_device,
        mesh=mesh,
        in_specs=(slab,) * 3 + (tile,) * 4,
        out_specs=(P(None, "gx", "gy"),) * 2,
        check_vma=False,
    )
```

```python
import jax
import jax.numpy as jnp
from jax import lax
from jax.experimental import pallas as pl
from jax.experimental.pallas import tpu as pltpu
from jax.sharding import PartitionSpec as P

gamma_ratio = 1.4
smooth_rate = 0.2
lift_rate = 0.3
couple_rate = 0.5
land_boost = 0.5

LEVELS, ROWS, COLS = 32, 128, 256
SLAB_ROWS, SLAB_COLS = 256, 2048
PIECE = 16
BAND = 16
QUARTER = ROWS // 4
EARLY = 2
MIB = 1024 * 1024
GATHER_MIB = 44


def remote(src, dst, send, recv, gx, gy):
    return pltpu.make_async_remote_copy(
        src, dst, send, recv, device_id={"gx": gx, "gy": gy}, device_id_type=pl.DeviceIdType.MESH
    )


def await_bytes(ref, sem):
    pltpu.make_async_copy(ref, ref, sem).wait()


def send_quarter(srcs, dsts, sends, recvs, quarter):
    gx, gy = lax.axis_index("gx"), lax.axis_index("gy")
    z, c, y = (gx // 2) % 4, gx % 2, gy % 4

    def piece(r, _):
        at = pl.multiple_of(r * PIECE, PIECE)
        for a in range(len(srcs)):
            for core in range(2):
                for shift in (0, 2, 1, 3):
                    for half in range(2):
                        c_to = (c + core) % 2
                        gx_to = gy * 2 + c_to
                        gy_to = half * 4 + (y + shift - z + 4) % 4
                        rows = pl.ds(pl.multiple_of(c_to * ROWS + at, PIECE), PIECE)
                        cols = pl.ds(pl.multiple_of(gy_to * COLS, COLS), COLS)

                        @pl.when(jnp.logical_not((gx_to == gx) & (gy_to == gy)))
                        def _():
                            remote(
                                srcs[a].at[:, rows, cols],
                                dsts[a].at[pl.ds(gx * 2, 2), pl.ds(at, PIECE)],
                                sends[a],
                                recvs[a],
                                gx_to,
                                gy_to,
                            ).start()
        return 0

    count = QUARTER // PIECE
    lax.fori_loop(quarter * count, quarter * count + count, piece, 0)


def smooth_wind(wind, smoothed):
    sub = lax.broadcasted_iota(jnp.int32, (8, SLAB_COLS), 0)
    lane = lax.broadcasted_iota(jnp.int32, (8, SLAB_COLS), 1)
    for level in range(2):

        def block(b, _):
            at = pl.multiple_of(b * 8, 8)
            before = wind[level, pl.ds(at, 8), :]
            here = wind[level, pl.ds(pl.multiple_of(at + 8, 8), 8), :]
            after = wind[level, pl.ds(pl.multiple_of(at + 16, 8), 8), :]
            low = jnp.where(sub == 0, pltpu.roll(before, 1, 0), pltpu.roll(here, 1, 0))
            high = jnp.where(sub == 7, pltpu.roll(after, 7, 0), pltpu.roll(here, 7, 0))
            left = jnp.where(lane == 0, 0.0, pltpu.roll(here, 1, 1))
            right = jnp.where(lane == SLAB_COLS - 1, 0.0, pltpu.roll(here, SLAB_COLS - 1, 1))
            lap = high + low + right + left - 4.0 * here
            smoothed[level, pl.ds(at, 8), :] = here + smooth_rate * lap
            return 0

        lax.fori_loop(0, SLAB_ROWS // 8, block, 0)


def columns(theta, press, terrain, mass, land, top, geo, couple, inverse, quarter):
    def band(b, _):
        rows = pl.ds(pl.multiple_of(b * BAND, BAND), BAND)
        ground, weight = terrain[rows, :], mass[rows, :]
        limit = jnp.where(land[rows, :] > 0, top[rows, :], 0)

        def state(k, rising):
            p = press[k, rows, :]
            alpha = theta[k, rows, :] * jnp.exp(-jnp.log(p) / gamma_ratio)
            rising = rising + alpha
            geo[k, rows, :] = ground + weight * rising / LEVELS
            return rising, gamma_ratio * p * alpha

        def eliminate(k, below, above, ratio):
            damping = jnp.where(k < limit, 1.0 + land_boost, 1.0)
            denom = damping + below + above - below * ratio
            inv = 1.0 / denom
            inverse[k, rows, :] = inv
            couple[k, rows, :] = above
            return above * inv

        def level(k, carry):
            rising, sound_low, below, ratio = carry
            rising, sound = state(k, rising)
            above = couple_rate * 0.5 * (sound_low + sound)
            ratio = eliminate(k - 1, below, above, ratio)
            return rising, sound, above, ratio

        zero = jnp.zeros((BAND, COLS), jnp.float32)
        rising, sound = state(0, zero)
        _, _, below, ratio = lax.fori_loop(1, LEVELS, level, (rising, sound, zero, zero))
        eliminate(LEVELS - 1, below, zero, ratio)
        return 0

    count = QUARTER // BAND
    lax.fori_loop(quarter * count, quarter * count + count, band, 0)


def pack_columns(geo, packed, quarter):
    rows = pl.ds(quarter * QUARTER, QUARTER)
    lane = lax.broadcasted_iota(jnp.int32, (QUARTER, 128), 1)
    base = quarter * LEVELS

    def level(k, carry):
        at = base + k
        last = pltpu.roll(geo[k, rows, COLS - 128 :], (at + 1) % 128, 1)
        first = pltpu.roll(geo[k, rows, :128], at, 1)
        return jnp.where(lane == at, last, carry[0]), jnp.where(lane == at, first, carry[1])

    carry = (jnp.zeros((QUARTER, 128), jnp.float32),) * 2 if quarter == 0 else (packed[0], packed[1])
    last, first = lax.fori_loop(0, LEVELS, level, carry)
    packed[0] = last
    packed[1] = first


def lift(geo, edge_rows, edge_cols, out):
    sub = lax.broadcasted_iota(jnp.int32, (ROWS, COLS), 0)
    lane = lax.broadcasted_iota(jnp.int32, (ROWS, 128), 1)

    def level(k, _):
        here = geo[k]
        low = jnp.where(sub == 0, edge_rows[0, k], pltpu.roll(here, 1, 0))
        high = jnp.where(sub == ROWS - 1, edge_rows[1, k], pltpu.roll(here, ROWS - 1, 0))
        left = pltpu.roll(here, 1, 1)
        right = pltpu.roll(here, COLS - 1, 1)
        west, east = edge_cols[0], edge_cols[1]
        from_left = jnp.concatenate(
            [pltpu.roll(west, (128 - LEVELS * q - k) % 128, 1) for q in range(4)], 0
        )
        from_right = jnp.concatenate(
            [pltpu.roll(east, 127 - LEVELS * q - k, 1) for q in range(4)], 0
        )
        for half in range(2):
            part = slice(half * 128, half * 128 + 128)
            l, r = left[:, part], right[:, part]
            if half == 0:
                l = jnp.where(lane == 0, from_left, l)
            else:
                r = jnp.where(lane == 127, from_right, r)
            lap = high[:, part] + low[:, part] + r + l - 4.0 * here[:, part]
            out[k, :, part] = lift_rate * lap
        return 0

    lax.fori_loop(0, LEVELS, level, 0)


def solve(wind, lifted, couple, inverse, quarter):
    rows = pl.ds(quarter * QUARTER, QUARTER)
    value = (wind[0, rows, :] + lifted[0, rows, :]) * inverse[0, rows, :]
    wind[0, rows, :] = value
    for k in range(1, LEVELS):
        below = couple[k - 1, rows, :]
        value = (wind[k, rows, :] + lifted[k, rows, :] + below * value) * inverse[k, rows, :]
        wind[k, rows, :] = value
    for k in range(LEVELS - 2, -1, -1):
        value = wind[k, rows, :] + couple[k, rows, :] * inverse[k, rows, :] * value
        wind[k, rows, :] = value


def gather(
    theta_in, press_in, wind_in, terrain_in, mass_in, land_in, top_in,
    forcing, geo,
    theta, press, wind, smoothed, lifted, couple, inverse, terrain, mass, land, top,
    edge_rows, edge_cols, packed, send, recv, edge_send, edge_recv, local,
):
    gx, gy = lax.axis_index("gx"), lax.axis_index("gy")
    c = gx % 2
    stays = (gx // 2) == gy
    moves = jnp.logical_not(stays)
    own_rows = pl.ds(pl.multiple_of(c * ROWS, ROWS), ROWS)
    own_cols = pl.ds(pl.multiple_of(gy * COLS, COLS), COLS)
    own_levels = pl.ds(gx * 2, 2)
    quarters = [pl.ds(q * QUARTER, QUARTER) for q in range(4)]
    low_x, high_x, low_y, high_y = gx > 0, gx < 15, gy > 0, gy < 7

    wind_up = remote(
        wind_in.at[:, pl.ds(SLAB_ROWS - 1, 1), :], wind.at[:, pl.ds(7, 1), :],
        edge_send.at[0], edge_recv.at[0], gx, (gy + 1) % 8,
    )
    wind_down = remote(
        wind_in.at[:, pl.ds(0, 1), :], wind.at[:, pl.ds(8 + SLAB_ROWS, 1), :],
        edge_send.at[1], edge_recv.at[1], gx, (gy + 7) % 8,
    )
    geo_up = remote(
        geo.at[:, pl.ds(ROWS - 1, 1), :], edge_rows.at[0],
        edge_send.at[2], edge_recv.at[2], (gx + 1) % 16, gy,
    )
    geo_down = remote(
        geo.at[:, pl.ds(0, 1), :], edge_rows.at[1],
        edge_send.at[3], edge_recv.at[3], (gx + 15) % 16, gy,
    )
    geo_right = remote(
        packed.at[0], edge_cols.at[0], edge_send.at[4], edge_recv.at[4], gx, (gy + 1) % 8
    )
    geo_left = remote(
        packed.at[1], edge_cols.at[1], edge_send.at[5], edge_recv.at[5], gx, (gy + 7) % 8
    )

    pl.when(high_y)(lambda: wind_up.start())
    pl.when(low_y)(lambda: wind_down.start())
    loads = [
        pltpu.make_async_copy(wind_in, wind.at[:, pl.ds(8, SLAB_ROWS), :], local.at[0]),
        pltpu.make_async_copy(terrain_in, terrain, local.at[1]),
        pltpu.make_async_copy(mass_in, mass, local.at[2]),
        pltpu.make_async_copy(land_in, land, local.at[3]),
        pltpu.make_async_copy(top_in, top, local.at[4]),
    ]
    own = [
        pltpu.make_async_copy(
            src.at[:, own_rows, own_cols], dst.at[own_levels], local.at[5 + a]
        )
        for a, (src, dst) in enumerate(((theta_in, theta), (press_in, press)))
    ]
    for load in loads:
        load.start()
    for load in loads:
        load.wait()

    @pl.when(stays)
    def _():
        for copy in own:
            copy.start()

    def send_state(q):
        send_quarter(
            (theta_in, press_in), (theta, press),
            (send.at[0], send.at[1]), (recv.at[q], recv.at[4 + q]), q,
        )

    def send_forcing(q):
        send_quarter((smoothed,), (forcing,), (send.at[2],), (recv.at[8 + q],), q)

    def await_quarter(refs, q):
        for count, cond in ((LEVELS - 2, stays), (LEVELS, moves)):

            @pl.when(cond)
            def _():
                for a, ref in refs:
                    await_bytes(ref.at[pl.ds(0, count), quarters[q]], recv.at[4 * a + q])

    send_state(0)

    blank = jnp.zeros((1, SLAB_COLS), jnp.float32)

    @pl.when(jnp.logical_not(low_y))
    def _():
        for level in range(2):
            wind[level, pl.ds(7, 1), :] = blank
        edge_cols[0] = jnp.zeros((QUARTER, 128), jnp.float32)

    @pl.when(jnp.logical_not(high_y))
    def _():
        for level in range(2):
            wind[level, pl.ds(8 + SLAB_ROWS, 1), :] = blank
        edge_cols[1] = jnp.zeros((QUARTER, 128), jnp.float32)

    @pl.when(jnp.logical_not(low_x))
    def _():
        edge_rows[0] = jnp.zeros((LEVELS, 1, COLS), jnp.float32)

    @pl.when(jnp.logical_not(high_x))
    def _():
        edge_rows[1] = jnp.zeros((LEVELS, 1, COLS), jnp.float32)

    pl.when(low_y)(lambda: wind_up.wait_recv())
    pl.when(high_y)(lambda: wind_down.wait_recv())
    smooth_wind(wind, smoothed)

    @pl.when(stays)
    def _():
        for level in range(2):
            forcing[gx * 2 + level] = smoothed[level, own_rows, own_cols]

    for q in range(1, 4):
        send_state(q)
    for q in range(EARLY):
        send_forcing(q)


    @pl.when(stays)
    def _():
        for copy in own:
            copy.wait()

    for q in range(4):
        await_quarter(((0, theta), (1, press)), q)
        columns(theta, press, terrain, mass, land, top, geo, couple, inverse, q)
        pack_columns(geo, packed, q)
        if q == 0:
            pl.when(low_x)(lambda: geo_down.start())
    pl.when(high_x)(lambda: geo_up.start())
    pl.when(high_y)(lambda: geo_right.start())
    pl.when(low_y)(lambda: geo_left.start())

    for q in range(EARLY, 4):
        send_forcing(q)

    pl.when(low_x)(lambda: geo_up.wait_recv())
    pl.when(high_x)(lambda: geo_down.wait_recv())

    pl.when(low_y)(lambda: geo_right.wait_recv())
    pl.when(high_y)(lambda: geo_left.wait_recv())
    lift(geo, edge_rows, edge_cols, lifted)
    for q in range(4):
        await_quarter(((2, forcing),), q)
        solve(forcing, lifted, couple, inverse, q)

    for cond, copies in (
        (high_x, (geo_up,)),
        (low_x, (geo_down,)),
        (high_y, (wind_up, geo_right)),
        (low_y, (wind_down, geo_left)),
    ):

        @pl.when(cond)
        def _():
            for copy in copies:
                copy.wait_send()

    for count, cond in ((LEVELS - 2, stays), (LEVELS, moves)):

        @pl.when(cond)
        def _():
            for a, ref in enumerate((theta, press, forcing)):
                await_bytes(ref.at[pl.ds(0, count)], send.at[a])


def store(wind, geo, wind_out, geo_out, sems):
    copies = []
    for n, (src, dst) in enumerate(((wind, wind_out), (geo, geo_out))):
        for part in range(4):
            levels = pl.ds(part * 8, 8)
            copies.append(pltpu.make_async_copy(src.at[levels], dst.at[levels], sems.at[n, part]))
    for copy in copies:
        copy.start()
    for copy in copies:
        copy.wait()


def on_device(*args):
    tile = jax.ShapeDtypeStruct((LEVELS, ROWS, COLS), jnp.float32)
    hbm = pl.BlockSpec(memory_space=pltpu.HBM)
    vmem = pl.BlockSpec(memory_space=pltpu.VMEM)
    f32, i32 = jnp.float32, jnp.int32
    parts = pl.pallas_call(
        gather,
        name="gather",
        out_shape=(tile,) * 2,
        in_specs=[hbm] * 7,
        out_specs=(vmem,) * 2,
        scratch_shapes=[
            pltpu.VMEM((LEVELS, ROWS, COLS), f32),
            pltpu.VMEM((LEVELS, ROWS, COLS), f32),
            pltpu.VMEM((2, SLAB_ROWS + 16, SLAB_COLS), f32),
            pltpu.VMEM((2, SLAB_ROWS, SLAB_COLS), f32),
            pltpu.VMEM((LEVELS, ROWS, COLS), f32),
            pltpu.VMEM((LEVELS, ROWS, COLS), f32),
            pltpu.VMEM((LEVELS, ROWS, COLS), f32),
            pltpu.VMEM((ROWS, COLS), f32),
            pltpu.VMEM((ROWS, COLS), f32),
            pltpu.VMEM((ROWS, COLS), i32),
            pltpu.VMEM((ROWS, COLS), i32),
            pltpu.VMEM((2, LEVELS, 1, COLS), f32),
            pltpu.VMEM((2, QUARTER, 128), f32),
            pltpu.VMEM((2, QUARTER, 128), f32),
            pltpu.SemaphoreType.DMA((3,)),
            pltpu.SemaphoreType.DMA((12,)),
            pltpu.SemaphoreType.DMA((6,)),
            pltpu.SemaphoreType.DMA((6,)),
            pltpu.SemaphoreType.DMA((7,)),
        ],
        compiler_params=pltpu.CompilerParams(
            has_side_effects=True, vmem_limit_bytes=GATHER_MIB * MIB
        ),
    )(*(pltpu.with_memory_space_constraint(x, pltpu.HBM) for x in args))
    return pl.pallas_call(
        store,
        name="store",
        out_shape=(tile, tile),
        in_specs=[vmem] * 2,
        out_specs=(hbm, hbm),
        scratch_shapes=[pltpu.SemaphoreType.DMA((2, 4))],
        compiler_params=pltpu.CompilerParams(vmem_limit_bytes=1 * MIB),
    )(*parts)


def solution(mesh):
    slab, tile = P("gx", "gy", None), P("gx", "gy")
    return jax.shard_map(
        on_device,
        mesh=mesh,
        in_specs=(slab,) * 3 + (tile,) * 4,
        out_specs=(P(None, "gx", "gy"),) * 2,
        check_vma=False,
    )
```

```python
import jax
import jax.numpy as jnp
from jax import lax
from jax.experimental import pallas as pl
from jax.experimental.pallas import tpu as pltpu
from jax.sharding import PartitionSpec as P

gamma_ratio = 1.4
smooth_rate = 0.2
lift_rate = 0.3
couple_rate = 0.5
land_boost = 0.5

LEVELS, ROWS, COLS = 32, 128, 256
SLAB_ROWS, SLAB_COLS = 256, 2048
PIECE = 8
BAND = 16
QUARTER = ROWS // 4
EARLY = 2
MIB = 1024 * 1024
GATHER_MIB = 44


def remote(src, dst, send, recv, gx, gy):
    return pltpu.make_async_remote_copy(
        src, dst, send, recv, device_id={"gx": gx, "gy": gy}, device_id_type=pl.DeviceIdType.MESH
    )


def await_bytes(ref, sem):
    pltpu.make_async_copy(ref, ref, sem).wait()


def send_quarter(srcs, dsts, sends, recvs, quarter):
    gx, gy = lax.axis_index("gx"), lax.axis_index("gy")
    z, c, y = (gx // 2) % 4, gx % 2, gy % 4

    def piece(r, _):
        at = pl.multiple_of(r * PIECE, PIECE)
        for a in range(len(srcs)):
            for core in range(2):
                for shift in (0, 2, 1, 3):
                    for half in range(2):
                        c_to = (c + core) % 2
                        gx_to = gy * 2 + c_to
                        gy_to = half * 4 + (y + shift - z + 4) % 4
                        rows = pl.ds(pl.multiple_of(c_to * ROWS + at, PIECE), PIECE)
                        cols = pl.ds(pl.multiple_of(gy_to * COLS, COLS), COLS)

                        @pl.when(jnp.logical_not((gx_to == gx) & (gy_to == gy)))
                        def _():
                            remote(
                                srcs[a].at[:, rows, cols],
                                dsts[a].at[pl.ds(gx * 2, 2), pl.ds(at, PIECE)],
                                sends[a],
                                recvs[a],
                                gx_to,
                                gy_to,
                            ).start()
        return 0

    count = QUARTER // PIECE
    lax.fori_loop(quarter * count, quarter * count + count, piece, 0)


def smooth_wind(wind, smoothed):
    sub = lax.broadcasted_iota(jnp.int32, (8, SLAB_COLS), 0)
    lane = lax.broadcasted_iota(jnp.int32, (8, SLAB_COLS), 1)
    for level in range(2):

        def block(b, _):
            at = pl.multiple_of(b * 8, 8)
            before = wind[level, pl.ds(at, 8), :]
            here = wind[level, pl.ds(pl.multiple_of(at + 8, 8), 8), :]
            after = wind[level, pl.ds(pl.multiple_of(at + 16, 8), 8), :]
            low = jnp.where(sub == 0, pltpu.roll(before, 1, 0), pltpu.roll(here, 1, 0))
            high = jnp.where(sub == 7, pltpu.roll(after, 7, 0), pltpu.roll(here, 7, 0))
            left = jnp.where(lane == 0, 0.0, pltpu.roll(here, 1, 1))
            right = jnp.where(lane == SLAB_COLS - 1, 0.0, pltpu.roll(here, SLAB_COLS - 1, 1))
            lap = high + low + right + left - 4.0 * here
            smoothed[level, pl.ds(at, 8), :] = here + smooth_rate * lap
            return 0

        lax.fori_loop(0, SLAB_ROWS // 8, block, 0)


def columns(theta, press, terrain, mass, land, top, geo, couple, inverse, quarter):
    def band(b, _):
        rows = pl.ds(pl.multiple_of(b * BAND, BAND), BAND)
        ground, weight = terrain[rows, :], mass[rows, :]
        limit = jnp.where(land[rows, :] > 0, top[rows, :], 0)

        def state(k, rising):
            p = press[k, rows, :]
            alpha = theta[k, rows, :] * jnp.exp(-jnp.log(p) / gamma_ratio)
            rising = rising + alpha
            geo[k, rows, :] = ground + weight * rising / LEVELS
            return rising, gamma_ratio * p * alpha

        def eliminate(k, below, above, ratio):
            damping = jnp.where(k < limit, 1.0 + land_boost, 1.0)
            denom = damping + below + above - below * ratio
            inv = 1.0 / denom
            inverse[k, rows, :] = inv
            couple[k, rows, :] = above
            return above * inv

        def level(k, carry):
            rising, sound_low, below, ratio = carry
            rising, sound = state(k, rising)
            above = couple_rate * 0.5 * (sound_low + sound)
            ratio = eliminate(k - 1, below, above, ratio)
            return rising, sound, above, ratio

        zero = jnp.zeros((BAND, COLS), jnp.float32)
        rising, sound = state(0, zero)
        _, _, below, ratio = lax.fori_loop(1, LEVELS, level, (rising, sound, zero, zero))
        eliminate(LEVELS - 1, below, zero, ratio)
        return 0

    count = QUARTER // BAND
    lax.fori_loop(quarter * count, quarter * count + count, band, 0)


def pack_columns(geo, packed, quarter):
    rows = pl.ds(quarter * QUARTER, QUARTER)
    lane = lax.broadcasted_iota(jnp.int32, (QUARTER, 128), 1)
    base = quarter * LEVELS

    def level(k, carry):
        at = base + k
        last = pltpu.roll(geo[k, rows, COLS - 128 :], (at + 1) % 128, 1)
        first = pltpu.roll(geo[k, rows, :128], at, 1)
        return jnp.where(lane == at, last, carry[0]), jnp.where(lane == at, first, carry[1])

    carry = (jnp.zeros((QUARTER, 128), jnp.float32),) * 2 if quarter == 0 else (packed[0], packed[1])
    last, first = lax.fori_loop(0, LEVELS, level, carry)
    packed[0] = last
    packed[1] = first


def lift(geo, edge_rows, edge_cols, out):
    sub = lax.broadcasted_iota(jnp.int32, (ROWS, COLS), 0)
    lane = lax.broadcasted_iota(jnp.int32, (ROWS, 128), 1)

    def level(k, _):
        here = geo[k]
        low = jnp.where(sub == 0, edge_rows[0, k], pltpu.roll(here, 1, 0))
        high = jnp.where(sub == ROWS - 1, edge_rows[1, k], pltpu.roll(here, ROWS - 1, 0))
        left = pltpu.roll(here, 1, 1)
        right = pltpu.roll(here, COLS - 1, 1)
        west, east = edge_cols[0], edge_cols[1]
        from_left = jnp.concatenate(
            [pltpu.roll(west, (128 - LEVELS * q - k) % 128, 1) for q in range(4)], 0
        )
        from_right = jnp.concatenate(
            [pltpu.roll(east, 127 - LEVELS * q - k, 1) for q in range(4)], 0
        )
        for half in range(2):
            part = slice(half * 128, half * 128 + 128)
            l, r = left[:, part], right[:, part]
            if half == 0:
                l = jnp.where(lane == 0, from_left, l)
            else:
                r = jnp.where(lane == 127, from_right, r)
            lap = high[:, part] + low[:, part] + r + l - 4.0 * here[:, part]
            out[k, :, part] = lift_rate * lap
        return 0

    lax.fori_loop(0, LEVELS, level, 0)


def solve(wind, lifted, couple, inverse, quarter):
    rows = pl.ds(quarter * QUARTER, QUARTER)
    value = (wind[0, rows, :] + lifted[0, rows, :]) * inverse[0, rows, :]
    wind[0, rows, :] = value
    for k in range(1, LEVELS):
        below = couple[k - 1, rows, :]
        value = (wind[k, rows, :] + lifted[k, rows, :] + below * value) * inverse[k, rows, :]
        wind[k, rows, :] = value
    for k in range(LEVELS - 2, -1, -1):
        value = wind[k, rows, :] + couple[k, rows, :] * inverse[k, rows, :] * value
        wind[k, rows, :] = value


def gather(
    theta_in, press_in, wind_in, terrain_in, mass_in, land_in, top_in,
    forcing, geo,
    theta, press, wind, smoothed, lifted, couple, inverse, terrain, mass, land, top,
    edge_rows, edge_cols, packed, send, recv, edge_send, edge_recv, local,
):
    gx, gy = lax.axis_index("gx"), lax.axis_index("gy")
    c = gx % 2
    stays = (gx // 2) == gy
    moves = jnp.logical_not(stays)
    own_rows = pl.ds(pl.multiple_of(c * ROWS, ROWS), ROWS)
    own_cols = pl.ds(pl.multiple_of(gy * COLS, COLS), COLS)
    own_levels = pl.ds(gx * 2, 2)
    quarters = [pl.ds(q * QUARTER, QUARTER) for q in range(4)]
    low_x, high_x, low_y, high_y = gx > 0, gx < 15, gy > 0, gy < 7

    wind_up = remote(
        wind_in.at[:, pl.ds(SLAB_ROWS - 1, 1), :], wind.at[:, pl.ds(7, 1), :],
        edge_send.at[0], edge_recv.at[0], gx, (gy + 1) % 8,
    )
    wind_down = remote(
        wind_in.at[:, pl.ds(0, 1), :], wind.at[:, pl.ds(8 + SLAB_ROWS, 1), :],
        edge_send.at[1], edge_recv.at[1], gx, (gy + 7) % 8,
    )
    geo_up = remote(
        geo.at[:, pl.ds(ROWS - 1, 1), :], edge_rows.at[0],
        edge_send.at[2], edge_recv.at[2], (gx + 1) % 16, gy,
    )
    geo_down = remote(
        geo.at[:, pl.ds(0, 1), :], edge_rows.at[1],
        edge_send.at[3], edge_recv.at[3], (gx + 15) % 16, gy,
    )
    geo_right = remote(
        packed.at[0], edge_cols.at[0], edge_send.at[4], edge_recv.at[4], gx, (gy + 1) % 8
    )
    geo_left = remote(
        packed.at[1], edge_cols.at[1], edge_send.at[5], edge_recv.at[5], gx, (gy + 7) % 8
    )

    pl.when(high_y)(lambda: wind_up.start())
    pl.when(low_y)(lambda: wind_down.start())
    loads = [
        pltpu.make_async_copy(wind_in, wind.at[:, pl.ds(8, SLAB_ROWS), :], local.at[0]),
        pltpu.make_async_copy(terrain_in, terrain, local.at[1]),
        pltpu.make_async_copy(mass_in, mass, local.at[2]),
        pltpu.make_async_copy(land_in, land, local.at[3]),
        pltpu.make_async_copy(top_in, top, local.at[4]),
    ]
    own = [
        pltpu.make_async_copy(
            src.at[:, own_rows, own_cols], dst.at[own_levels], local.at[5 + a]
        )
        for a, (src, dst) in enumerate(((theta_in, theta), (press_in, press)))
    ]
    for load in loads:
        load.start()
    for load in loads:
        load.wait()

    @pl.when(stays)
    def _():
        for copy in own:
            copy.start()

    def send_state(q):
        send_quarter(
            (theta_in, press_in), (theta, press),
            (send.at[0], send.at[1]), (recv.at[q], recv.at[4 + q]), q,
        )

    def send_forcing(q):
        send_quarter((smoothed,), (forcing,), (send.at[2],), (recv.at[8 + q],), q)

    def await_quarter(refs, q):
        for count, cond in ((LEVELS - 2, stays), (LEVELS, moves)):

            @pl.when(cond)
            def _():
                for a, ref in refs:
                    await_bytes(ref.at[pl.ds(0, count), quarters[q]], recv.at[4 * a + q])

    send_state(0)

    blank = jnp.zeros((1, SLAB_COLS), jnp.float32)

    @pl.when(jnp.logical_not(low_y))
    def _():
        for level in range(2):
            wind[level, pl.ds(7, 1), :] = blank
        edge_cols[0] = jnp.zeros((QUARTER, 128), jnp.float32)

    @pl.when(jnp.logical_not(high_y))
    def _():
        for level in range(2):
            wind[level, pl.ds(8 + SLAB_ROWS, 1), :] = blank
        edge_cols[1] = jnp.zeros((QUARTER, 128), jnp.float32)

    @pl.when(jnp.logical_not(low_x))
    def _():
        edge_rows[0] = jnp.zeros((LEVELS, 1, COLS), jnp.float32)

    @pl.when(jnp.logical_not(high_x))
    def _():
        edge_rows[1] = jnp.zeros((LEVELS, 1, COLS), jnp.float32)

    pl.when(low_y)(lambda: wind_up.wait_recv())
    pl.when(high_y)(lambda: wind_down.wait_recv())
    smooth_wind(wind, smoothed)

    @pl.when(stays)
    def _():
        for level in range(2):
            forcing[gx * 2 + level] = smoothed[level, own_rows, own_cols]

    for q in range(1, 4):
        send_state(q)
    for q in range(EARLY):
        send_forcing(q)


    @pl.when(stays)
    def _():
        for copy in own:
            copy.wait()

    for q in range(4):
        await_quarter(((0, theta), (1, press)), q)
        columns(theta, press, terrain, mass, land, top, geo, couple, inverse, q)
        pack_columns(geo, packed, q)
        if q == 0:
            pl.when(low_x)(lambda: geo_down.start())
    pl.when(high_x)(lambda: geo_up.start())
    pl.when(high_y)(lambda: geo_right.start())
    pl.when(low_y)(lambda: geo_left.start())

    for q in range(EARLY, 4):
        send_forcing(q)

    pl.when(low_x)(lambda: geo_up.wait_recv())
    pl.when(high_x)(lambda: geo_down.wait_recv())

    pl.when(low_y)(lambda: geo_right.wait_recv())
    pl.when(high_y)(lambda: geo_left.wait_recv())
    lift(geo, edge_rows, edge_cols, lifted)
    for q in range(4):
        await_quarter(((2, forcing),), q)
        solve(forcing, lifted, couple, inverse, q)

    for cond, copies in (
        (high_x, (geo_up,)),
        (low_x, (geo_down,)),
        (high_y, (wind_up, geo_right)),
        (low_y, (wind_down, geo_left)),
    ):

        @pl.when(cond)
        def _():
            for copy in copies:
                copy.wait_send()

    for count, cond in ((LEVELS - 2, stays), (LEVELS, moves)):

        @pl.when(cond)
        def _():
            for a, ref in enumerate((theta, press, forcing)):
                await_bytes(ref.at[pl.ds(0, count)], send.at[a])


def store(wind, geo, wind_out, geo_out, sems):
    copies = []
    for n, (src, dst) in enumerate(((wind, wind_out), (geo, geo_out))):
        for part in range(4):
            levels = pl.ds(part * 8, 8)
            copies.append(pltpu.make_async_copy(src.at[levels], dst.at[levels], sems.at[n, part]))
    for copy in copies:
        copy.start()
    for copy in copies:
        copy.wait()


def on_device(*args):
    tile = jax.ShapeDtypeStruct((LEVELS, ROWS, COLS), jnp.float32)
    hbm = pl.BlockSpec(memory_space=pltpu.HBM)
    vmem = pl.BlockSpec(memory_space=pltpu.VMEM)
    f32, i32 = jnp.float32, jnp.int32
    parts = pl.pallas_call(
        gather,
        name="gather",
        out_shape=(tile,) * 2,
        in_specs=[hbm] * 7,
        out_specs=(vmem,) * 2,
        scratch_shapes=[
            pltpu.VMEM((LEVELS, ROWS, COLS), f32),
            pltpu.VMEM((LEVELS, ROWS, COLS), f32),
            pltpu.VMEM((2, SLAB_ROWS + 16, SLAB_COLS), f32),
            pltpu.VMEM((2, SLAB_ROWS, SLAB_COLS), f32),
            pltpu.VMEM((LEVELS, ROWS, COLS), f32),
            pltpu.VMEM((LEVELS, ROWS, COLS), f32),
            pltpu.VMEM((LEVELS, ROWS, COLS), f32),
            pltpu.VMEM((ROWS, COLS), f32),
            pltpu.VMEM((ROWS, COLS), f32),
            pltpu.VMEM((ROWS, COLS), i32),
            pltpu.VMEM((ROWS, COLS), i32),
            pltpu.VMEM((2, LEVELS, 1, COLS), f32),
            pltpu.VMEM((2, QUARTER, 128), f32),
            pltpu.VMEM((2, QUARTER, 128), f32),
            pltpu.SemaphoreType.DMA((3,)),
            pltpu.SemaphoreType.DMA((12,)),
            pltpu.SemaphoreType.DMA((6,)),
            pltpu.SemaphoreType.DMA((6,)),
            pltpu.SemaphoreType.DMA((7,)),
        ],
        compiler_params=pltpu.CompilerParams(
            has_side_effects=True, vmem_limit_bytes=GATHER_MIB * MIB
        ),
    )(*(pltpu.with_memory_space_constraint(x, pltpu.HBM) for x in args))
    return pl.pallas_call(
        store,
        name="store",
        out_shape=(tile, tile),
        in_specs=[vmem] * 2,
        out_specs=(hbm, hbm),
        scratch_shapes=[pltpu.SemaphoreType.DMA((2, 4))],
        compiler_params=pltpu.CompilerParams(vmem_limit_bytes=1 * MIB),
    )(*parts)


def solution(mesh):
    slab, tile = P("gx", "gy", None), P("gx", "gy")
    return jax.shard_map(
        on_device,
        mesh=mesh,
        in_specs=(slab,) * 3 + (tile,) * 4,
        out_specs=(P(None, "gx", "gy"),) * 2,
        check_vma=False,
    )
```
